32 devices in a mesh: vox: 8 (over z, core), sta: 4 (over y, x).
Axes of the slice: x: 2, y: 2, z: 4, core: 2. Of those that a mesh axis runs over, the one named last changes fastest.
Arguments:
- green_tensor: bfloat16 [4, 6, 256, 1024], P('sta', None, None, 'vox'), may hold values from -0.078125 to 0.078125
- strain: bfloat16 [8, 6, 256, 1024], P('sta', None, None, 'vox'), may hold values from -6 to 6
- pair_events: int32 [4, 8], P('sta'), may hold values from -1 to 7, as said below
- pair_counts: int32 [4], P('sta'), may hold values from 6 to 8, as said below
- residuals: float32 [4, 8, 256], P('sta'), may hold values from -0.375 to 0.375
Outputs:
- kernel: float32 [1024], P(('vox', 'sta'))
The draws below stay inside these ranges and needn't reach their ends.
Inputs may be any that keep to these rules, and one draw needn't show every extreme that they name: `pair_events`: within a station the live entries are distinct earthquakes; slots at or beyond the station's count hold -1. `pair_counts`: some station has exactly 8 live slots in every draw.
All inputs are finite; a program needn't handle non-finite values.
Results may differ from the reference program's by a relative error of at most 0.0029.
Values may be sent and summed in bfloat16 or wider, within the bound.
A program may use at most 64 MiB of HBM per device.

```python
import jax
import jax.numpy as jnp
from jax import lax

COMP = 6
NT = 256
STATIONS = 4
EVENTS = 8
MAXP = 8
VOX = 1024


def pair_lists(key):
    first = jax.random.fold_in(key, 11)
    second = jax.random.fold_in(key, 12)
    third = jax.random.fold_in(key, 13)
    orders = jax.vmap(lambda k: jax.random.permutation(k, EVENTS))(jax.random.split(first, STATIONS))[:, :MAXP]
    drawn = jax.random.randint(second, (STATIONS,), 0, MAXP // 3 + 1)
    counts = MAXP - drawn
    busiest = jax.random.randint(third, (), 0, STATIONS)
    counts = jnp.where(jnp.arange(STATIONS) == busiest, MAXP, counts).astype(jnp.int32)
    places = jnp.arange(MAXP)[None, :]
    events = jnp.where(places < counts[:, None], orders, -1).astype(jnp.int32)
    return (events, counts)


def draw_pair_events(key, part):
    return pair_lists(key)[0]


def draw_pair_counts(key, part):
    return pair_lists(key)[1]


def shard_levels(own_key, shape, shards, smallest, top_value):
    factor_of = 1.0
    for dim, shards_of in shards:
        steps = jax.random.uniform(jax.random.fold_in(jax.random.fold_in(own_key, 6), dim), (shards_of,), jnp.float32, smallest / len(shards), top_value / len(shards))
        factor_of = factor_of * jnp.repeat(jnp.exp(steps), shape[dim] // shards_of).reshape((-1,) + (1,) * (len(shape) - 1 - dim))
    return factor_of


def noise(rng, shape, scale, bound, cuts=(), kind=jnp.bfloat16):
    array = scale * jax.random.normal(rng, shape, jnp.float32)
    if cuts:
        array = array * shard_levels(rng, shape, cuts, -0.22, 0.18)
    return jnp.clip(array, -bound, bound).astype(kind)


def setup_inputs(seed: int = 0) -> dict:
    arg_keys = jax.random.split(jax.random.key(seed), 6)
    return {
        "green_tensor": noise(arg_keys[0], (STATIONS, COMP, NT, VOX), (4 * COMP * NT) ** -0.5, 0.078125, ((0, 4), (3, 8))),
        "strain": noise(arg_keys[1], (EVENTS, COMP, NT, VOX), 1.0, 6.0, ((0, 4), (3, 8))),
        "pair_events": draw_pair_events(jax.random.fold_in(arg_keys[5], 71), 0),
        "pair_counts": draw_pair_counts(jax.random.fold_in(arg_keys[5], 71), 0),
        "residuals": noise(arg_keys[4], (STATIONS, MAXP, NT), NT ** -0.5, 0.375, ((0, 4),), jnp.float32),
    }


def toeplitz(wave):
    steps = jnp.arange(NT, dtype=jnp.int32)
    offset = steps[:, None] - steps[None, :]
    values = jnp.take(wave, jnp.clip(offset, 0, NT - 1), axis=-1)
    return jnp.where(offset >= 0, values, jnp.zeros_like(values))


def reference(green_tensor, strain, pair_events, pair_counts, residuals):
    def station(total, index):
        green = green_tensor[index].astype(jnp.float32)

        def slot(acc, place):
            event = pair_events[index, place]
            live = place < pair_counts[index]
            field = lax.dynamic_index_in_dim(strain, jnp.maximum(event, 0).astype(jnp.int32), 0, keepdims=False)
            matrix = toeplitz(residuals[index, place]).astype(jnp.bfloat16)
            conv = jnp.einsum("tu,cuv->ctv", matrix.astype(jnp.float32), field.astype(jnp.float32))
            term = jnp.sum(green * conv, axis=(0, 1))
            return acc + jnp.where(live, term, jnp.zeros_like(term)), None

        acc, _ = lax.scan(slot, total, jnp.arange(MAXP, dtype=jnp.int32))
        return acc, None

    start = jnp.zeros((VOX,), jnp.float32)
    kernel, _ = lax.scan(station, start, jnp.arange(STATIONS, dtype=jnp.int32))
    return kernel
```

```python
import functools

import jax
import jax.numpy as jnp
from jax import lax
from jax.experimental import pallas as pl
from jax.experimental.pallas import tpu as pltpu
from jax.sharding import PartitionSpec as P

LANES = 128
F32 = jnp.float32
BF16 = jnp.bfloat16


def kernel(
    n, events_ref, counts_ref, resid_ref, green_hbm, strain_hbm, out_ref,
    green, strain, packed_green, packed_strain, all_comb, all_green, all_strain, adjoint,
    load_sem, send_sem, recv_sem,
):
    me = lax.axis_index("sta")
    comps, nt, vox = green.shape
    local_events = strain.shape[0]
    slots = resid_ref.shape[0]
    width = vox // n
    per_tile = LANES // width
    full = comps // per_tile
    rest = comps % per_tile
    fit = min(per_tile // rest, local_events) if rest else 1
    blocks = nt // LANES

    def peer(d):
        pair = lax.rem(me // 2 + d // 2, n // 2)
        return 2 * pair + lax.rem(me + d, 2)

    order = list(range(n - 1, 0, -1))
    load_green = pltpu.make_async_copy(green_hbm.at[0], green, load_sem.at[0])
    load_strain = pltpu.make_async_copy(strain_hbm, strain, load_sem.at[1])
    load_green.start()
    load_strain.start()

    barrier = pltpu.get_barrier_semaphore()
    for d in order:
        pl.semaphore_signal(
            barrier, inc=1, device_id={"sta": peer(d)}, device_id_type=pl.DeviceIdType.MESH
        )

    def send(kind, src, dst, d):
        copy = pltpu.make_async_remote_copy(
            src_ref=src,
            dst_ref=dst.at[me],
            send_sem=send_sem.at[kind, d],
            recv_sem=recv_sem.at[kind, me],
            device_id={"sta": peer(d)},
            device_id_type=pl.DeviceIdType.MESH,
        )
        copy.start()
        return copy

    def wait_from(kind, dst, j):
        pltpu.make_async_remote_copy(
            src_ref=dst.at[j],
            dst_ref=dst.at[j],
            send_sem=send_sem.at[kind, 0],
            recv_sem=recv_sem.at[kind, j],
            device_id={"sta": j},
            device_id_type=pl.DeviceIdType.MESH,
        ).wait_recv()

    rows = lax.broadcasted_iota(jnp.int32, (all_comb.shape[1], nt), 0)
    comb = jnp.zeros((all_comb.shape[1], nt), F32)
    for p in range(slots):
        event = jnp.where(p < counts_ref[0], events_ref[0, p], -1)
        comb = comb + jnp.where(rows == event, resid_ref[p : p + 1, :], 0.0)
    all_comb[me] = comb

    lane = lax.broadcasted_iota(jnp.int32, (LANES, LANES), 0)
    column = lax.broadcasted_iota(jnp.int32, (LANES, LANES), 1)

    def pick(j, slot):
        inside = (column >= slot * width) & (column < (slot + 1) * width)
        return inside & (lane == column + (j - slot) * width)

    def as_matrix(masks):
        return jnp.concatenate([jnp.where(m, 1.0, 0.0).astype(BF16) for m in masks], axis=0)

    def gathered(tiles, matrix):
        wide = jnp.concatenate(tiles, axis=1)
        return jnp.dot(wide, matrix[: len(tiles) * LANES], preferred_element_type=F32).astype(BF16)

    def pack_green(j, masks, matrix, dst, index):
        for a in range(full):
            dst[index, a] = gathered([green[a * per_tile + k] for k in range(per_tile)], matrix)
        if rest:
            repeated = []
            for k in range(rest):
                hit = masks[k]
                for i in range(1, fit):
                    hit = hit | masks[i * rest + k]
                repeated.append(hit)
            dst[index, full] = gathered(
                [green[full * per_tile + k] for k in range(rest)], as_matrix(repeated)
            )

    def pack_strain(matrix, dst, index):
        tile = 0
        for e in range(local_events):
            for a in range(full):
                dst[index, tile] = gathered(
                    [strain[e, a * per_tile + k] for k in range(per_tile)], matrix
                )
                tile += 1
        if rest:
            for e in range(0, local_events, fit):
                dst[index, tile] = gathered(
                    [strain[e + i, full * per_tile + k] for i in range(fit) for k in range(rest)],
                    matrix,
                )
                tile += 1

    matrices = {}
    for d in order + [0]:
        j = peer(d)
        masks = [pick(j, slot) for slot in range(per_tile)]
        matrices[d] = (j, masks, as_matrix(masks))

    load_green.wait()
    copies = []
    pl.semaphore_wait(barrier, n - 1)
    for d in order:
        copies.append(send(0, all_comb.at[me], all_comb, d))
    waiting = None
    for d in order:
        pack_green(*matrices[d], packed_green, d)
        if waiting is not None:
            copies.append(send(1, packed_green.at[waiting], all_green, waiting))
        waiting = d
    pack_green(*matrices[0], all_green, me)
    copies.append(send(1, packed_green.at[waiting], all_green, waiting))
    load_strain.wait()
    waiting = None
    for d in order:
        pack_strain(matrices[d][2], packed_strain, d)
        if waiting is not None:
            copies.append(send(2, packed_strain.at[waiting], all_strain, waiting))
        waiting = d
    pack_strain(matrices[0][2], all_strain, me)
    copies.append(send(2, packed_strain.at[waiting], all_strain, waiting))

    for d in order:
        wait_from(0, all_comb, peer(d))
    for d in order:
        wait_from(1, all_green, peer(d))

    later = column >= lane
    nothing = jnp.zeros((LANES, LANES), BF16)
    tiles = all_green.shape[1]

    @pl.loop(0, all_comb.shape[1])
    def _(e):
        total = jnp.zeros((nt, tiles * LANES), F32)
        for s in range(n):
            wave = all_comb[s, pl.ds(e, 1), :]
            turned = []
            for k in range(blocks):
                piece = jnp.broadcast_to(wave[:, k * LANES : (k + 1) * LANES], (LANES, LANES))
                turned.append(pltpu.roll(piece, 0, 1, stride=1, stride_axis=0))
            diag = [
                jnp.where(later, turned[k], turned[k - 1] if k else 0.0).astype(BF16)
                for k in range(blocks)
            ]
            matrix = jnp.concatenate(
                [
                    jnp.concatenate([nothing] * i + diag[: blocks - i], axis=1)
                    for i in range(blocks)
                ],
                axis=0,
            )
            field = jnp.concatenate([all_green[s, t] for t in range(tiles)], axis=1)
            total = total + jnp.dot(matrix, field, preferred_element_type=F32)
        adjoint[e] = total

    spot = lax.broadcasted_iota(jnp.int32, (nt, LANES), 1)

    def meet(j):
        part = jnp.zeros((1, LANES), F32)
        tile = 0
        for e in range(local_events):
            for a in range(full):
                field = all_strain[j, tile].astype(F32)
                one = adjoint[j * local_events + e, :, a * LANES : (a + 1) * LANES]
                part = part + jnp.sum(field * one, axis=0, keepdims=True)
                tile += 1
        if rest:
            for e in range(0, local_events, fit):
                field = all_strain[j, tile].astype(F32)
                one = adjoint[j * local_events + e, :, full * LANES :]
                for i in range(1, fit):
                    other = adjoint[j * local_events + e + i, :, full * LANES :]
                    one = jnp.where(spot < i * rest * width, one, other)
                part = part + jnp.sum(
                    jnp.where(spot < fit * rest * width, field * one, 0.0), axis=0, keepdims=True
                )
                tile += 1
        return part

    answer = meet(me)
    for d in order:
        j = peer(d)
        wait_from(2, all_strain, j)
        answer = answer + meet(j)
    total = answer[:, :width]
    for k in range(1, per_tile):
        total = total + answer[:, k * width : (k + 1) * width]
    out_ref[...] = total
    for copy in copies:
        copy.wait_send()


def solution(mesh):
    n = mesh.shape["sta"]

    def body(green_tensor, strain, pair_events, pair_counts, residuals):
        _, comps, nt, vox = green_tensor.shape
        local_events = strain.shape[0]
        width = vox // n
        per_tile = LANES // width
        full = comps // per_tile
        rest = comps % per_tile
        fit = min(per_tile // rest, local_events) if rest else 1
        green_tiles = full + (1 if rest else 0)
        strain_tiles = full * local_events + (local_events // fit if rest else 0)
        events = n * local_events
        out = pl.pallas_call(
            functools.partial(kernel, n),
            out_shape=jax.ShapeDtypeStruct((1, width), F32),
            in_specs=[
                pl.BlockSpec(memory_space=pltpu.SMEM),
                pl.BlockSpec(memory_space=pltpu.SMEM),
                pl.BlockSpec(memory_space=pltpu.VMEM),
                pl.BlockSpec(memory_space=pl.ANY),
                pl.BlockSpec(memory_space=pl.ANY),
            ],
            out_specs=pl.BlockSpec(memory_space=pltpu.VMEM),
            scratch_shapes=[
                pltpu.VMEM((comps, nt, vox), BF16),
                pltpu.VMEM((local_events, comps, nt, vox), BF16),
                pltpu.VMEM((n, green_tiles, nt, LANES), BF16),
                pltpu.VMEM((n, strain_tiles, nt, LANES), BF16),
                pltpu.VMEM((n, events, nt), F32),
                pltpu.VMEM((n, green_tiles, nt, LANES), BF16),
                pltpu.VMEM((n, strain_tiles, nt, LANES), BF16),
                pltpu.VMEM((events, nt, green_tiles * LANES), F32),
                pltpu.SemaphoreType.DMA((2,)),
                pltpu.SemaphoreType.DMA((3, n)),
                pltpu.SemaphoreType.DMA((3, n)),
            ],
            compiler_params=pltpu.CompilerParams(collective_id=0, has_side_effects=True),
        )(pair_events, pair_counts, residuals[0], green_tensor, strain)
        return out[0]

    in_specs = (
        P("sta", None, None, "vox"),
        P("sta", None, None, "vox"),
        P("sta", None),
        P("sta"),
        P("sta", None, None),
    )
    out_specs = P(("vox", "sta"))
    return jax.shard_map(body, mesh=mesh, in_specs=in_specs, out_specs=out_specs, check_vma=False)
```

```python
import functools

import jax
import jax.numpy as jnp
from jax import lax
from jax.experimental import pallas as pl
from jax.experimental.pallas import tpu as pltpu
from jax.sharding import PartitionSpec as P

LANES = 128
F32 = jnp.float32
BF16 = jnp.bfloat16


def kernel(
    n, events_ref, counts_ref, resid_ref, green_hbm, strain_hbm, out_ref,
    green, strain, packed_green, packed_strain, all_comb, all_green, all_strain, adjoint,
    load_sem, send_sem, recv_sem,
):
    me = lax.axis_index("sta")
    comps, nt, vox = green.shape
    local_events = strain.shape[0]
    slots = resid_ref.shape[0]
    width = vox // n
    per_tile = LANES // width
    full = comps // per_tile
    rest = comps % per_tile
    fit = min(per_tile // rest, local_events) if rest else 1
    blocks = nt // LANES

    def peer(d):
        pair = lax.rem(me // 2 + d // 2, n // 2)
        return 2 * pair + lax.rem(me + d, 2)

    order = list(range(n - 1, 0, -1))
    load_green = pltpu.make_async_copy(green_hbm.at[0], green, load_sem.at[0])
    load_strain = pltpu.make_async_copy(strain_hbm, strain, load_sem.at[1])
    load_green.start()
    load_strain.start()

    barrier = pltpu.get_barrier_semaphore()
    for d in order:
        pl.semaphore_signal(
            barrier, inc=1, device_id={"sta": peer(d)}, device_id_type=pl.DeviceIdType.MESH
        )

    def send(kind, src, dst, d):
        copy = pltpu.make_async_remote_copy(
            src_ref=src,
            dst_ref=dst.at[me],
            send_sem=send_sem.at[kind, d],
            recv_sem=recv_sem.at[kind, me],
            device_id={"sta": peer(d)},
            device_id_type=pl.DeviceIdType.MESH,
        )
        copy.start()
        return copy

    def wait_from(kind, dst, j):
        pltpu.make_async_remote_copy(
            src_ref=dst.at[j],
            dst_ref=dst.at[j],
            send_sem=send_sem.at[kind, 0],
            recv_sem=recv_sem.at[kind, j],
            device_id={"sta": j},
            device_id_type=pl.DeviceIdType.MESH,
        ).wait_recv()

    rows = lax.broadcasted_iota(jnp.int32, (all_comb.shape[1], nt), 0)
    comb = jnp.zeros((all_comb.shape[1], nt), F32)
    for p in range(slots):
        event = jnp.where(p < counts_ref[0], events_ref[0, p], -1)
        comb = comb + jnp.where(rows == event, resid_ref[p : p + 1, :], 0.0)
    all_comb[me] = comb

    lane = lax.broadcasted_iota(jnp.int32, (LANES, LANES), 0)
    column = lax.broadcasted_iota(jnp.int32, (LANES, LANES), 1)

    def pick(j, slot):
        inside = (column >= slot * width) & (column < (slot + 1) * width)
        return inside & (lane == column + (j - slot) * width)

    def as_matrix(masks):
        return jnp.concatenate([jnp.where(m, 1.0, 0.0).astype(BF16) for m in masks], axis=0)

    def gathered(tiles, matrix):
        wide = jnp.concatenate(tiles, axis=1)
        return jnp.dot(wide, matrix[: len(tiles) * LANES], preferred_element_type=F32).astype(BF16)

    def pack_green(j, masks, matrix, dst, index):
        for a in range(full):
            dst[index, a] = gathered([green[a * per_tile + k] for k in range(per_tile)], matrix)
        if rest:
            repeated = []
            for k in range(rest):
                hit = masks[k]
                for i in range(1, fit):
                    hit = hit | masks[i * rest + k]
                repeated.append(hit)
            dst[index, full] = gathered(
                [green[full * per_tile + k] for k in range(rest)], as_matrix(repeated)
            )

    def pack_strain(matrix, dst, index):
        tile = 0
        for e in range(local_events):
            for a in range(full):
                dst[index, tile] = gathered(
                    [strain[e, a * per_tile + k] for k in range(per_tile)], matrix
                )
                tile += 1
        if rest:
            for e in range(0, local_events, fit):
                dst[index, tile] = gathered(
                    [strain[e + i, full * per_tile + k] for i in range(fit) for k in range(rest)],
                    matrix,
                )
                tile += 1

    matrices = {}
    for d in order + [0]:
        j = peer(d)
        masks = [pick(j, slot) for slot in range(per_tile)]
        matrices[d] = (j, masks, as_matrix(masks))

    load_green.wait()
    copies = []
    pl.semaphore_wait(barrier, n - 1)
    for d in order:
        copies.append(send(0, all_comb.at[me], all_comb, d))
    waiting = None
    for d in order:
        pack_green(*matrices[d], packed_green, d)
        if waiting is not None:
            copies.append(send(1, packed_green.at[waiting], all_green, waiting))
        waiting = d
    pack_green(*matrices[0], all_green, me)
    copies.append(send(1, packed_green.at[waiting], all_green, waiting))
    load_strain.wait()
    waiting = None
    for d in order:
        pack_strain(matrices[d][2], packed_strain, d)
        if waiting is not None:
            copies.append(send(2, packed_strain.at[waiting], all_strain, waiting))
        waiting = d
    pack_strain(matrices[0][2], all_strain, me)
    copies.append(send(2, packed_strain.at[waiting], all_strain, waiting))

    for d in order:
        wait_from(0, all_comb, peer(d))
    for d in order:
        wait_from(1, all_green, peer(d))

    later = column >= lane
    nothing = jnp.zeros((LANES, LANES), BF16)
    tiles = all_green.shape[1]

    @pl.loop(0, all_comb.shape[1])
    def _(e):
        total = jnp.zeros((nt, tiles * LANES), F32)
        for s in range(n):
            wave = all_comb[s, pl.ds(e, 1), :]
            turned = []
            for k in range(blocks):
                piece = jnp.broadcast_to(wave[:, k * LANES : (k + 1) * LANES], (LANES, LANES))
                turned.append(pltpu.roll(piece, 0, 1, stride=1, stride_axis=0))
            diag = [
                jnp.where(later, turned[k], turned[k - 1] if k else 0.0).astype(BF16)
                for k in range(blocks)
            ]
            matrix = jnp.concatenate(
                [
                    jnp.concatenate([nothing] * i + diag[: blocks - i], axis=1)
                    for i in range(blocks)
                ],
                axis=0,
            )
            field = jnp.concatenate([all_green[s, t] for t in range(tiles)], axis=1)
            total = total + jnp.dot(matrix, field, preferred_element_type=F32)
        adjoint[e] = total

    spot = lax.broadcasted_iota(jnp.int32, (nt, LANES), 1)

    def meet(j):
        part = jnp.zeros((1, LANES), F32)
        tile = 0
        for e in range(local_events):
            for a in range(full):
                field = all_strain[j, tile].astype(F32)
                one = adjoint[j * local_events + e, :, a * LANES : (a + 1) * LANES]
                part = part + jnp.sum(field * one, axis=0, keepdims=True)
                tile += 1
        if rest:
            for e in range(0, local_events, fit):
                field = all_strain[j, tile].astype(F32)
                one = adjoint[j * local_events + e, :, full * LANES :]
                for i in range(1, fit):
                    other = adjoint[j * local_events + e + i, :, full * LANES :]
                    one = jnp.where(spot < i * rest * width, one, other)
                part = part + jnp.sum(
                    jnp.where(spot < fit * rest * width, field * one, 0.0), axis=0, keepdims=True
                )
                tile += 1
        return part

    answer = meet(me)
    for d in order:
        j = peer(d)
        wait_from(2, all_strain, j)
        answer = answer + meet(j)
    total = answer[:, :width]
    for k in range(1, per_tile):
        total = total + answer[:, k * width : (k + 1) * width]
    out_ref[...] = total[0]
    for copy in copies:
        copy.wait_send()


def square_kernel(
    events_ref, counts_ref, resid_ref, green_hbm, strain_hbm, out_ref,
    green, strain, send_green, send_strain, own_green, far_green, own_strain, far_strain,
    own_tail, far_tail, waves, own_adjoint, far_adjoint, part_out, part_in,
    load_sem, send_sem, recv_sem,
):
    me = lax.axis_index("sta")
    x, y = lax.rem(me, 2), me // 2
    odd = lax.rem(x + y, 2)
    beside = me + 1 - 2 * x
    above = lax.rem(me + 2, 4)
    first = beside + odd * (above - beside)
    second = above + odd * (beside - above)
    across = 3 - me
    comps, nt, vox = green.shape
    local_events = strain.shape[0]
    width = vox // 4
    per_tile = LANES // width
    full = comps // per_tile
    rest = comps % per_tile
    blocks = nt // LANES
    head = full * nt

    load_green = pltpu.make_async_copy(green_hbm.at[0], green, load_sem.at[0])
    load_strain = pltpu.make_async_copy(strain_hbm, strain, load_sem.at[1])
    load_green.start()
    load_strain.start()

    barrier = pltpu.get_barrier_semaphore()
    for target in (first, second, across):
        pl.semaphore_signal(
            barrier, inc=1, device_id={"sta": target}, device_id_type=pl.DeviceIdType.MESH
        )

    def copy_of(kind, src, dst, target):
        return pltpu.make_async_remote_copy(
            src_ref=src,
            dst_ref=dst,
            send_sem=send_sem.at[kind],
            recv_sem=recv_sem.at[kind],
            device_id={"sta": target},
            device_id_type=pl.DeviceIdType.MESH,
        )

    plan = {
        "wave1": copy_of(0, waves.at[0], waves.at[2], first),
        "wave2": copy_of(1, waves.at[0], waves.at[1], second),
        "wave3": copy_of(2, waves.at[0], waves.at[3], across),
        "u0": copy_of(3, send_green.at[0], far_green.at[2], first),
        "u1": copy_of(4, send_strain.at[0], far_strain.at[1], first),
        "u2": copy_of(5, far_green.at[0], own_green.at[2], first),
        "u3": copy_of(6, far_green.at[2], own_green.at[3], first),
        "w0": copy_of(7, own_green.at[0], far_green.at[1], second),
        "w1": copy_of(8, send_green.at[1], own_green.at[1], second),
        "w2": copy_of(9, send_strain.at[1, 0], own_strain.at[1, 0], second),
        "w3": copy_of(10, send_strain.at[1, 1:], own_strain.at[1, 1:], second),
        "w4": copy_of(11, own_green.at[1], far_green.at[3], second),
        "sum": copy_of(12, part_out, part_in, first),
    }

    events = waves.shape[1]
    rows = lax.broadcasted_iota(jnp.int32, (events, nt), 0)
    comb = jnp.zeros((events, nt), F32)
    for p in range(resid_ref.shape[0]):
        event = jnp.where(p < counts_ref[0], events_ref[0, p], -1)
        comb = comb + jnp.where(rows == event, resid_ref[p : p + 1, :], 0.0)
    waves[0] = comb

    lane = lax.broadcasted_iota(jnp.int32, (LANES, LANES), 0)
    column = lax.broadcasted_iota(jnp.int32, (LANES, LANES), 1)

    def picker(j):
        parts = []
        for slot in range(per_tile):
            inside = (column >= slot * width) & (column < (slot + 1) * width)
            hit = inside & (lane == column + (j - slot) * width)
            parts.append(jnp.where(hit, 1.0, 0.0).astype(BF16))
        return jnp.concatenate(parts, axis=0)

    def gathered(pieces, matrix):
        wide = jnp.concatenate(pieces, axis=1)
        return jnp.dot(wide, matrix, preferred_element_type=F32).astype(BF16)

    def pack_green(matrix, dst, index):
        for a in range(full):
            dst[index, a * nt : (a + 1) * nt] = gathered(
                [green[a * per_tile + k] for k in range(per_tile)], matrix
            )
        half = nt // 2
        dst[index, head : head + half] = gathered(
            [green[full * per_tile + k, h * half : (h + 1) * half] for h in range(2) for k in range(rest)],
            matrix,
        )

    def pack_strain(matrix, dst, index):
        tile = 0
        for e in range(local_events):
            for a in range(full):
                dst[index, tile] = gathered(
                    [strain[e, a * per_tile + k] for k in range(per_tile)], matrix
                )
                tile += 1
        dst[index, tile] = gathered(
            [strain[i, full * per_tile + k] for i in range(local_events) for k in range(rest)],
            matrix,
        )

    to_across, to_me, to_second, to_first = (picker(j) for j in (across, me, second, first))
    pl.semaphore_wait(barrier, 3)
    for name in ("wave3", "wave1", "wave2"):
        plan[name].start()
    load_green.wait()
    pack_green(to_across, send_green, 0)
    pack_green(to_me, own_green, 0)
    plan["u0"].start()
    pack_green(to_second, send_green, 1)
    plan["w0"].start()
    load_strain.wait()
    pack_strain(to_across, send_strain, 0)
    plan["w1"].start()
    pack_green(to_first, far_green, 0)
    plan["u1"].start()
    pack_strain(to_second, send_strain, 1)
    plan["u2"].start()
    pack_strain(to_first, far_strain, 0)
    plan["w2"].start()
    pack_strain(to_me, own_strain, 0)

    later = column >= lane
    low = column < rest * width
    nothing = jnp.zeros((LANES, LANES), BF16)

    def unfold(source, s, dst):
        half = nt // 2
        for b in range(half // LANES):
            piece = source[s, head + b * LANES : head + (b + 1) * LANES].astype(F32)
            turned = pltpu.roll(piece, LANES // 2, 1)
            dst[s, b * LANES : (b + 1) * LANES] = jnp.where(low, piece, turned).astype(BF16)
            dst[s, half + b * LANES : half + (b + 1) * LANES] = jnp.where(
                low, turned, piece
            ).astype(BF16)

    def toeplitz(s, row):
        wave = waves[s, pl.ds(row, 1), :]
        turned = []
        for k in range(blocks):
            piece = jnp.broadcast_to(wave[:, k * LANES : (k + 1) * LANES], (LANES, LANES))
            turned.append(pltpu.roll(piece, 0, 1, stride=1, stride_axis=0))
        diag = [
            jnp.where(later, turned[k], turned[k - 1] if k else 0.0).astype(BF16)
            for k in range(blocks)
        ]
        return jnp.concatenate(
            [jnp.concatenate([nothing] * i + diag[: blocks - i], axis=1) for i in range(blocks)],
            axis=0,
        )

    def advance(source, tail, adjoint, partner, stations, fresh):
        for s in stations:
            unfold(source, s, tail)

        @pl.loop(0, 2 * local_events)
        def _(k):
            row = me * local_events + k + (k // local_events) * (partner - me - 1) * local_events
            total = jnp.zeros(adjoint.shape[1:], F32) if fresh else adjoint[k]
            for s in stations:
                field = jnp.concatenate(
                    [source[s, a * nt : (a + 1) * nt] for a in range(full)] + [tail[s]], axis=1
                )
                total = total + jnp.dot(toeplitz(s, row), field, preferred_element_type=F32)
            adjoint[k] = total

    spot = lax.broadcasted_iota(jnp.int32, (nt, LANES), 1)

    def meet(field, adjoint, side):
        part = jnp.zeros((1, LANES), F32)
        tile = 0
        base = side * local_events
        for e in range(local_events):
            for a in range(full):
                one = adjoint[base + e, :, a * LANES : (a + 1) * LANES]
                part = part + jnp.sum(field[side, tile].astype(F32) * one, axis=0, keepdims=True)
                tile += 1
        one = adjoint[base, :, full * LANES :]
        for i in range(1, local_events):
            one = jnp.where(spot < i * rest * width, one, adjoint[base + i, :, full * LANES :])
        return part + jnp.sum(field[side, tile].astype(F32) * one, axis=0, keepdims=True)

    plan["u0"].wait_recv()
    plan["u3"].start()
    for name in ("wave1", "wave2", "wave3", "w0"):
        plan[name].wait_recv()
    advance(far_green, far_tail, far_adjoint, second, (0, 1, 2), True)
    plan["w1"].wait_recv()
    plan["w4"].start()
    plan["w3"].start()
    advance(own_green, own_tail, own_adjoint, first, (0, 1), True)
    plan["w4"].wait_recv()
    advance(far_green, far_tail, far_adjoint, second, (3,), False)
    part = meet(far_strain, far_adjoint, 0)
    plan["u1"].wait_recv()
    part_out[...] = part + meet(far_strain, far_adjoint, 1)
    plan["u2"].wait_recv()
    advance(own_green, own_tail, own_adjoint, first, (2,), False)
    plan["sum"].start()
    plan["u3"].wait_recv()
    advance(own_green, own_tail, own_adjoint, first, (3,), False)
    answer = meet(own_strain, own_adjoint, 0)
    plan["w2"].wait_recv()
    plan["w3"].wait_recv()
    answer = answer + meet(own_strain, own_adjoint, 1)
    plan["sum"].wait_recv()
    answer = answer + part_in[...]
    total = answer[:, :width]
    for k in range(1, per_tile):
        total = total + answer[:, k * width : (k + 1) * width]
    out_ref[...] = total[0]
    for copy in plan.values():
        copy.wait_send()


def solution(mesh):
    n = mesh.shape["sta"]

    def body(green_tensor, strain, pair_events, pair_counts, residuals):
        _, comps, nt, vox = green_tensor.shape
        local_events = strain.shape[0]
        width = vox // n
        per_tile = LANES // width
        full = comps // per_tile
        rest = comps % per_tile
        fit = min(per_tile // rest, local_events) if rest else 1
        green_tiles = full + (1 if rest else 0)
        strain_tiles = full * local_events + (local_events // fit if rest else 0)
        events = n * local_events
        packed = full * nt + nt // 2
        if n == 4 and 2 * rest == per_tile and local_events * rest == per_tile:
            steps = square_kernel
            scratch = [
                pltpu.VMEM((comps, nt, vox), BF16),
                pltpu.VMEM((local_events, comps, nt, vox), BF16),
                pltpu.VMEM((2, packed, LANES), BF16),
                pltpu.VMEM((2, strain_tiles, nt, LANES), BF16),
                pltpu.VMEM((4, packed, LANES), BF16),
                pltpu.VMEM((4, packed, LANES), BF16),
                pltpu.VMEM((2, strain_tiles, nt, LANES), BF16),
                pltpu.VMEM((2, strain_tiles, nt, LANES), BF16),
                pltpu.VMEM((4, nt, LANES), BF16),
                pltpu.VMEM((4, nt, LANES), BF16),
                pltpu.VMEM((4, events, nt), F32),
                pltpu.VMEM((2 * local_events, nt, green_tiles * LANES), F32),
                pltpu.VMEM((2 * local_events, nt, green_tiles * LANES), F32),
                pltpu.VMEM((1, LANES), F32),
                pltpu.VMEM((1, LANES), F32),
                pltpu.SemaphoreType.DMA((2,)),
                pltpu.SemaphoreType.DMA((13,)),
                pltpu.SemaphoreType.DMA((13,)),
            ]
        else:
            steps = functools.partial(kernel, n)
            scratch = [
                pltpu.VMEM((comps, nt, vox), BF16),
                pltpu.VMEM((local_events, comps, nt, vox), BF16),
                pltpu.VMEM((n, green_tiles, nt, LANES), BF16),
                pltpu.VMEM((n, strain_tiles, nt, LANES), BF16),
                pltpu.VMEM((n, events, nt), F32),
                pltpu.VMEM((n, green_tiles, nt, LANES), BF16),
                pltpu.VMEM((n, strain_tiles, nt, LANES), BF16),
                pltpu.VMEM((events, nt, green_tiles * LANES), F32),
                pltpu.SemaphoreType.DMA((2,)),
                pltpu.SemaphoreType.DMA((3, n)),
                pltpu.SemaphoreType.DMA((3, n)),
            ]
        return pl.pallas_call(
            steps,
            out_shape=jax.ShapeDtypeStruct((width,), F32),
            in_specs=[
                pl.BlockSpec(memory_space=pltpu.SMEM),
                pl.BlockSpec(memory_space=pltpu.SMEM),
                pl.BlockSpec(memory_space=pltpu.VMEM),
                pl.BlockSpec(memory_space=pl.ANY),
                pl.BlockSpec(memory_space=pl.ANY),
            ],
            out_specs=pl.BlockSpec(memory_space=pltpu.VMEM),
            scratch_shapes=scratch,
            compiler_params=pltpu.CompilerParams(collective_id=0, has_side_effects=True),
        )(pair_events, pair_counts, residuals[0], green_tensor, strain)

    in_specs = (
        P("sta", None, None, "vox"),
        P("sta", None, None, "vox"),
        P("sta", None),
        P("sta"),
        P("sta", None, None),
    )
    out_specs = P(("vox", "sta"))
    return jax.shard_map(body, mesh=mesh, in_specs=in_specs, out_specs=out_specs, check_vma=False)
```

```python
import functools

import jax
import jax.numpy as jnp
from jax import lax
from jax.experimental import pallas as pl
from jax.experimental.pallas import tpu as pltpu
from jax.sharding import PartitionSpec as P

LANES = 128
F32 = jnp.float32
BF16 = jnp.bfloat16


def kernel(
    n, events_ref, counts_ref, resid_ref, green_hbm, strain_hbm, out_ref,
    green, strain, packed_green, packed_strain, all_comb, all_green, all_strain, adjoint,
    load_sem, send_sem, recv_sem,
):
    me = lax.axis_index("sta")
    comps, nt, vox = green.shape
    local_events = strain.shape[0]
    slots = resid_ref.shape[0]
    width = vox // n
    per_tile = LANES // width
    full = comps // per_tile
    rest = comps % per_tile
    fit = min(per_tile // rest, local_events) if rest else 1
    blocks = nt // LANES

    def peer(d):
        pair = lax.rem(me // 2 + d // 2, n // 2)
        return 2 * pair + lax.rem(me + d, 2)

    order = list(range(n - 1, 0, -1))
    load_green = pltpu.make_async_copy(green_hbm.at[0], green, load_sem.at[0])
    load_strain = pltpu.make_async_copy(strain_hbm, strain, load_sem.at[1])
    load_green.start()
    load_strain.start()

    barrier = pltpu.get_barrier_semaphore()
    for d in order:
        pl.semaphore_signal(
            barrier, inc=1, device_id={"sta": peer(d)}, device_id_type=pl.DeviceIdType.MESH
        )

    def send(kind, src, dst, d):
        copy = pltpu.make_async_remote_copy(
            src_ref=src,
            dst_ref=dst.at[me],
            send_sem=send_sem.at[kind, d],
            recv_sem=recv_sem.at[kind, me],
            device_id={"sta": peer(d)},
            device_id_type=pl.DeviceIdType.MESH,
        )
        copy.start()
        return copy

    def wait_from(kind, dst, j):
        pltpu.make_async_remote_copy(
            src_ref=dst.at[j],
            dst_ref=dst.at[j],
            send_sem=send_sem.at[kind, 0],
            recv_sem=recv_sem.at[kind, j],
            device_id={"sta": j},
            device_id_type=pl.DeviceIdType.MESH,
        ).wait_recv()

    rows = lax.broadcasted_iota(jnp.int32, (all_comb.shape[1], nt), 0)
    comb = jnp.zeros((all_comb.shape[1], nt), F32)
    for p in range(slots):
        event = jnp.where(p < counts_ref[0], events_ref[0, p], -1)
        comb = comb + jnp.where(rows == event, resid_ref[p : p + 1, :], 0.0)
    all_comb[me] = comb

    lane = lax.broadcasted_iota(jnp.int32, (LANES, LANES), 0)
    column = lax.broadcasted_iota(jnp.int32, (LANES, LANES), 1)

    def pick(j, slot):
        inside = (column >= slot * width) & (column < (slot + 1) * width)
        return inside & (lane == column + (j - slot) * width)

    def as_matrix(masks):
        return jnp.concatenate([jnp.where(m, 1.0, 0.0).astype(BF16) for m in masks], axis=0)

    def gathered(tiles, matrix):
        wide = jnp.concatenate(tiles, axis=1)
        return jnp.dot(wide, matrix[: len(tiles) * LANES], preferred_element_type=F32).astype(BF16)

    def pack_green(j, masks, matrix, dst, index):
        for a in range(full):
            dst[index, a] = gathered([green[a * per_tile + k] for k in range(per_tile)], matrix)
        if rest:
            repeated = []
            for k in range(rest):
                hit = masks[k]
                for i in range(1, fit):
                    hit = hit | masks[i * rest + k]
                repeated.append(hit)
            dst[index, full] = gathered(
                [green[full * per_tile + k] for k in range(rest)], as_matrix(repeated)
            )

    def pack_strain(matrix, dst, index):
        tile = 0
        for e in range(local_events):
            for a in range(full):
                dst[index, tile] = gathered(
                    [strain[e, a * per_tile + k] for k in range(per_tile)], matrix
                )
                tile += 1
        if rest:
            for e in range(0, local_events, fit):
                dst[index, tile] = gathered(
                    [strain[e + i, full * per_tile + k] for i in range(fit) for k in range(rest)],
                    matrix,
                )
                tile += 1

    matrices = {}
    for d in order + [0]:
        j = peer(d)
        masks = [pick(j, slot) for slot in range(per_tile)]
        matrices[d] = (j, masks, as_matrix(masks))

    load_green.wait()
    copies = []
    pl.semaphore_wait(barrier, n - 1)
    for d in order:
        copies.append(send(0, all_comb.at[me], all_comb, d))
    waiting = None
    for d in order:
        pack_green(*matrices[d], packed_green, d)
        if waiting is not None:
            copies.append(send(1, packed_green.at[waiting], all_green, waiting))
        waiting = d
    pack_green(*matrices[0], all_green, me)
    copies.append(send(1, packed_green.at[waiting], all_green, waiting))
    load_strain.wait()
    waiting = None
    for d in order:
        pack_strain(matrices[d][2], packed_strain, d)
        if waiting is not None:
            copies.append(send(2, packed_strain.at[waiting], all_strain, waiting))
        waiting = d
    pack_strain(matrices[0][2], all_strain, me)
    copies.append(send(2, packed_strain.at[waiting], all_strain, waiting))

    for d in order:
        wait_from(0, all_comb, peer(d))
    for d in order:
        wait_from(1, all_green, peer(d))

    later = column >= lane
    nothing = jnp.zeros((LANES, LANES), BF16)
    tiles = all_green.shape[1]

    @pl.loop(0, all_comb.shape[1])
    def _(e):
        total = jnp.zeros((nt, tiles * LANES), F32)
        for s in range(n):
            wave = all_comb[s, pl.ds(e, 1), :]
            turned = []
            for k in range(blocks):
                piece = jnp.broadcast_to(wave[:, k * LANES : (k + 1) * LANES], (LANES, LANES))
                turned.append(pltpu.roll(piece, 0, 1, stride=1, stride_axis=0))
            diag = [
                jnp.where(later, turned[k], turned[k - 1] if k else 0.0).astype(BF16)
                for k in range(blocks)
            ]
            matrix = jnp.concatenate(
                [
                    jnp.concatenate([nothing] * i + diag[: blocks - i], axis=1)
                    for i in range(blocks)
                ],
                axis=0,
            )
            field = jnp.concatenate([all_green[s, t] for t in range(tiles)], axis=1)
            total = total + jnp.dot(matrix, field, preferred_element_type=F32)
        adjoint[e] = total

    spot = lax.broadcasted_iota(jnp.int32, (nt, LANES), 1)

    def meet(j):
        part = jnp.zeros((1, LANES), F32)
        tile = 0
        for e in range(local_events):
            for a in range(full):
                field = all_strain[j, tile].astype(F32)
                one = adjoint[j * local_events + e, :, a * LANES : (a + 1) * LANES]
                part = part + jnp.sum(field * one, axis=0, keepdims=True)
                tile += 1
        if rest:
            for e in range(0, local_events, fit):
                field = all_strain[j, tile].astype(F32)
                one = adjoint[j * local_events + e, :, full * LANES :]
                for i in range(1, fit):
                    other = adjoint[j * local_events + e + i, :, full * LANES :]
                    one = jnp.where(spot < i * rest * width, one, other)
                part = part + jnp.sum(
                    jnp.where(spot < fit * rest * width, field * one, 0.0), axis=0, keepdims=True
                )
                tile += 1
        return part

    answer = meet(me)
    for d in order:
        j = peer(d)
        wait_from(2, all_strain, j)
        answer = answer + meet(j)
    total = answer[:, :width]
    for k in range(1, per_tile):
        total = total + answer[:, k * width : (k + 1) * width]
    out_ref[...] = total[0]
    for copy in copies:
        copy.wait_send()


def square_kernel(
    events_ref, counts_ref, resid_ref, green_hbm, strain_hbm, out_ref,
    green, strain, send_green, send_strain, own_green, far_green, own_strain, far_strain,
    own_tail, far_tail, waves, own_adjoint, far_adjoint, part_out, part_in,
    load_sem, send_sem, recv_sem,
):
    me = lax.axis_index("sta")
    x, y = lax.rem(me, 2), me // 2
    odd = lax.rem(x + y, 2)
    beside = me + 1 - 2 * x
    above = lax.rem(me + 2, 4)
    first = beside + odd * (above - beside)
    second = above + odd * (beside - above)
    across = 3 - me
    comps, nt, vox = green.shape
    local_events = strain.shape[0]
    width = vox // 4
    per_tile = LANES // width
    full = comps // per_tile
    rest = comps % per_tile
    blocks = nt // LANES
    head = full * nt

    load_green = pltpu.make_async_copy(green_hbm.at[0], green, load_sem.at[0])
    load_strain = pltpu.make_async_copy(strain_hbm, strain, load_sem.at[1])
    load_green.start()
    load_strain.start()

    barrier = pltpu.get_barrier_semaphore()
    for target in (first, second, across):
        pl.semaphore_signal(
            barrier, inc=1, device_id={"sta": target}, device_id_type=pl.DeviceIdType.MESH
        )

    def copy_of(kind, src, dst, target):
        return pltpu.make_async_remote_copy(
            src_ref=src,
            dst_ref=dst,
            send_sem=send_sem.at[kind],
            recv_sem=recv_sem.at[kind],
            device_id={"sta": target},
            device_id_type=pl.DeviceIdType.MESH,
        )

    plan = {
        "wave1": copy_of(0, waves.at[0], waves.at[2], first),
        "wave2": copy_of(1, waves.at[0], waves.at[1], second),
        "wave3": copy_of(2, waves.at[0], waves.at[3], across),
        "u0": copy_of(3, send_green.at[0], far_green.at[2], first),
        "u1": copy_of(4, send_strain.at[0], far_strain.at[1], first),
        "u2": copy_of(5, far_green.at[0], own_green.at[2], first),
        "u3": copy_of(6, far_green.at[2], own_green.at[3], first),
        "w0": copy_of(7, own_green.at[0], far_green.at[1], second),
        "w1": copy_of(8, send_green.at[1], own_green.at[1], second),
        "w2": copy_of(9, send_strain.at[1], own_strain.at[1], second),
        "w4": copy_of(10, own_green.at[1], far_green.at[3], second),
        "sum": copy_of(11, part_out, part_in, first),
    }

    events = waves.shape[1]
    rows = lax.broadcasted_iota(jnp.int32, (events, nt), 0)
    comb = jnp.zeros((events, nt), F32)
    for p in range(resid_ref.shape[0]):
        event = jnp.where(p < counts_ref[0], events_ref[0, p], -1)
        comb = comb + jnp.where(rows == event, resid_ref[p : p + 1, :], 0.0)
    waves[0] = comb

    lane = lax.broadcasted_iota(jnp.int32, (LANES, LANES), 0)
    column = lax.broadcasted_iota(jnp.int32, (LANES, LANES), 1)

    def picker(j):
        parts = []
        for slot in range(per_tile):
            inside = (column >= slot * width) & (column < (slot + 1) * width)
            hit = inside & (lane == column + (j - slot) * width)
            parts.append(jnp.where(hit, 1.0, 0.0).astype(BF16))
        return jnp.concatenate(parts, axis=0)

    def gathered(pieces, matrix):
        wide = jnp.concatenate(pieces, axis=1)
        return jnp.dot(wide, matrix, preferred_element_type=F32).astype(BF16)

    def pack_green(matrix, dst, index):
        for a in range(full):
            dst[index, a * nt : (a + 1) * nt] = gathered(
                [green[a * per_tile + k] for k in range(per_tile)], matrix
            )
        half = nt // 2
        dst[index, head : head + half] = gathered(
            [green[full * per_tile + k, h * half : (h + 1) * half] for h in range(2) for k in range(rest)],
            matrix,
        )

    def pack_strain(matrix, dst, index):
        tile = 0
        for e in range(local_events):
            for a in range(full):
                dst[index, tile] = gathered(
                    [strain[e, a * per_tile + k] for k in range(per_tile)], matrix
                )
                tile += 1
        dst[index, tile] = gathered(
            [strain[i, full * per_tile + k] for i in range(local_events) for k in range(rest)],
            matrix,
        )

    to_across, to_second = picker(across), picker(second)
    load_green.wait()
    pack_green(to_across, send_green, 0)
    pack_green(to_second, send_green, 1)
    to_me, to_first = picker(me), picker(first)
    pl.semaphore_wait(barrier, 3)
    plan["u0"].start()
    plan["w1"].start()
    for name in ("wave3", "wave1", "wave2"):
        plan[name].start()
    load_strain.wait()
    pack_strain(to_across, send_strain, 0)
    pack_green(to_me, own_green, 0)
    plan["u1"].start()
    pack_green(to_first, far_green, 0)
    plan["w0"].start()
    pack_strain(to_second, send_strain, 1)
    plan["u2"].start()

    later = column >= lane
    low = column < rest * width
    nothing = jnp.zeros((LANES, LANES), BF16)

    def unfold(source, s, dst):
        half = nt // 2
        for b in range(half // LANES):
            piece = source[s, head + b * LANES : head + (b + 1) * LANES].astype(F32)
            turned = pltpu.roll(piece, LANES // 2, 1)
            dst[s, b * LANES : (b + 1) * LANES] = jnp.where(low, piece, turned).astype(BF16)
            dst[s, half + b * LANES : half + (b + 1) * LANES] = jnp.where(
                low, turned, piece
            ).astype(BF16)

    def toeplitz(s, row):
        wave = waves[s, pl.ds(row, 1), :]
        turned = []
        for k in range(blocks):
            piece = jnp.broadcast_to(wave[:, k * LANES : (k + 1) * LANES], (LANES, LANES))
            turned.append(pltpu.roll(piece, 0, 1, stride=1, stride_axis=0))
        diag = [
            jnp.where(later, turned[k], turned[k - 1] if k else 0.0).astype(BF16)
            for k in range(blocks)
        ]
        return jnp.concatenate(
            [jnp.concatenate([nothing] * i + diag[: blocks - i], axis=1) for i in range(blocks)],
            axis=0,
        )

    def advance(source, tail, adjoint, partner, stations, fresh):
        for s in stations:
            unfold(source, s, tail)

        @pl.loop(0, 2 * local_events)
        def _(k):
            row = me * local_events + k + (k // local_events) * (partner - me - 1) * local_events
            total = jnp.zeros(adjoint.shape[1:], F32) if fresh else adjoint[k]
            for s in stations:
                field = jnp.concatenate(
                    [source[s, a * nt : (a + 1) * nt] for a in range(full)] + [tail[s]], axis=1
                )
                total = total + jnp.dot(toeplitz(s, row), field, preferred_element_type=F32)
            adjoint[k] = total

    spot = lax.broadcasted_iota(jnp.int32, (nt, LANES), 1)

    def meet(field, adjoint, side):
        part = jnp.zeros((1, LANES), F32)
        tile = 0
        base = side * local_events
        for e in range(local_events):
            for a in range(full):
                one = adjoint[base + e, :, a * LANES : (a + 1) * LANES]
                part = part + jnp.sum(field[side, tile].astype(F32) * one, axis=0, keepdims=True)
                tile += 1
        one = adjoint[base, :, full * LANES :]
        for i in range(1, local_events):
            one = jnp.where(spot < i * rest * width, one, adjoint[base + i, :, full * LANES :])
        return part + jnp.sum(field[side, tile].astype(F32) * one, axis=0, keepdims=True)

    plan["u0"].wait_recv()
    plan["u3"].start()
    plan["w1"].wait_recv()
    plan["w4"].start()
    plan["w2"].start()
    pack_strain(to_first, far_strain, 0)
    pack_strain(to_me, own_strain, 0)
    for name in ("wave1", "wave2", "wave3"):
        plan[name].wait_recv()
    advance(own_green, own_tail, own_adjoint, first, (0, 1), True)
    plan["w0"].wait_recv()
    advance(far_green, far_tail, far_adjoint, second, (0, 1, 2), True)
    plan["w4"].wait_recv()
    advance(far_green, far_tail, far_adjoint, second, (3,), False)
    part = meet(far_strain, far_adjoint, 0)
    plan["u1"].wait_recv()
    part_out[...] = part + meet(far_strain, far_adjoint, 1)
    plan["u2"].wait_recv()
    advance(own_green, own_tail, own_adjoint, first, (2,), False)
    plan["sum"].start()
    plan["u3"].wait_recv()
    advance(own_green, own_tail, own_adjoint, first, (3,), False)
    answer = meet(own_strain, own_adjoint, 0)
    plan["w2"].wait_recv()
    answer = answer + meet(own_strain, own_adjoint, 1)
    plan["sum"].wait_recv()
    answer = answer + part_in[...]
    total = answer[:, :width]
    for k in range(1, per_tile):
        total = total + answer[:, k * width : (k + 1) * width]
    out_ref[...] = total[0]
    for copy in plan.values():
        copy.wait_send()


def solution(mesh):
    n = mesh.shape["sta"]

    def body(green_tensor, strain, pair_events, pair_counts, residuals):
        _, comps, nt, vox = green_tensor.shape
        local_events = strain.shape[0]
        width = vox // n
        per_tile = LANES // width
        full = comps // per_tile
        rest = comps % per_tile
        fit = min(per_tile // rest, local_events) if rest else 1
        green_tiles = full + (1 if rest else 0)
        strain_tiles = full * local_events + (local_events // fit if rest else 0)
        events = n * local_events
        packed = full * nt + nt // 2
        if n == 4 and 2 * rest == per_tile and local_events * rest == per_tile:
            steps = square_kernel
            scratch = [
                pltpu.VMEM((comps, nt, vox), BF16),
                pltpu.VMEM((local_events, comps, nt, vox), BF16),
                pltpu.VMEM((2, packed, LANES), BF16),
                pltpu.VMEM((2, strain_tiles, nt, LANES), BF16),
                pltpu.VMEM((4, packed, LANES), BF16),
                pltpu.VMEM((4, packed, LANES), BF16),
                pltpu.VMEM((2, strain_tiles, nt, LANES), BF16),
                pltpu.VMEM((2, strain_tiles, nt, LANES), BF16),
                pltpu.VMEM((4, nt, LANES), BF16),
                pltpu.VMEM((4, nt, LANES), BF16),
                pltpu.VMEM((4, events, nt), F32),
                pltpu.VMEM((2 * local_events, nt, green_tiles * LANES), F32),
                pltpu.VMEM((2 * local_events, nt, green_tiles * LANES), F32),
                pltpu.VMEM((1, LANES), F32),
                pltpu.VMEM((1, LANES), F32),
                pltpu.SemaphoreType.DMA((2,)),
                pltpu.SemaphoreType.DMA((12,)),
                pltpu.SemaphoreType.DMA((12,)),
            ]
        else:
            steps = functools.partial(kernel, n)
            scratch = [
                pltpu.VMEM((comps, nt, vox), BF16),
                pltpu.VMEM((local_events, comps, nt, vox), BF16),
                pltpu.VMEM((n, green_tiles, nt, LANES), BF16),
                pltpu.VMEM((n, strain_tiles, nt, LANES), BF16),
                pltpu.VMEM((n, events, nt), F32),
                pltpu.VMEM((n, green_tiles, nt, LANES), BF16),
                pltpu.VMEM((n, strain_tiles, nt, LANES), BF16),
                pltpu.VMEM((events, nt, green_tiles * LANES), F32),
                pltpu.SemaphoreType.DMA((2,)),
                pltpu.SemaphoreType.DMA((3, n)),
                pltpu.SemaphoreType.DMA((3, n)),
            ]
        return pl.pallas_call(
            steps,
            out_shape=jax.ShapeDtypeStruct((width,), F32),
            in_specs=[
                pl.BlockSpec(memory_space=pltpu.SMEM),
                pl.BlockSpec(memory_space=pltpu.SMEM),
                pl.BlockSpec(memory_space=pltpu.VMEM),
                pl.BlockSpec(memory_space=pl.ANY),
                pl.BlockSpec(memory_space=pl.ANY),
            ],
            out_specs=pl.BlockSpec(memory_space=pltpu.VMEM),
            scratch_shapes=scratch,
            compiler_params=pltpu.CompilerParams(collective_id=0, has_side_effects=True),
        )(pair_events, pair_counts, residuals[0], green_tensor, strain)

    in_specs = (
        P("sta", None, None, "vox"),
        P("sta", None, None, "vox"),
        P("sta", None),
        P("sta"),
        P("sta", None, None),
    )
    out_specs = P(("vox", "sta"))
    return jax.shard_map(body, mesh=mesh, in_specs=in_specs, out_specs=out_specs, check_vma=False)
```

```python
import functools

import jax
import jax.numpy as jnp
from jax import lax
from jax.experimental import pallas as pl
from jax.experimental.pallas import tpu as pltpu
from jax.sharding import PartitionSpec as P

LANES = 128
F32 = jnp.float32
BF16 = jnp.bfloat16


def kernel(
    n, events_ref, counts_ref, resid_ref, green_hbm, strain_hbm, out_ref,
    green, strain, packed_green, packed_strain, all_comb, all_green, all_strain, adjoint,
    load_sem, send_sem, recv_sem,
):
    me = lax.axis_index("sta")
    comps, nt, vox = green.shape
    local_events = strain.shape[0]
    slots = resid_ref.shape[0]
    width = vox // n
    per_tile = LANES // width
    full = comps // per_tile
    rest = comps % per_tile
    fit = min(per_tile // rest, local_events) if rest else 1
    blocks = nt // LANES

    def peer(d):
        pair = lax.rem(me // 2 + d // 2, n // 2)
        return 2 * pair + lax.rem(me + d, 2)

    order = list(range(n - 1, 0, -1))
    load_green = pltpu.make_async_copy(green_hbm.at[0], green, load_sem.at[0])
    load_strain = pltpu.make_async_copy(strain_hbm, strain, load_sem.at[1])
    load_green.start()
    load_strain.start()

    barrier = pltpu.get_barrier_semaphore()
    for d in order:
        pl.semaphore_signal(
            barrier, inc=1, device_id={"sta": peer(d)}, device_id_type=pl.DeviceIdType.MESH
        )

    def send(kind, src, dst, d):
        copy = pltpu.make_async_remote_copy(
            src_ref=src,
            dst_ref=dst.at[me],
            send_sem=send_sem.at[kind, d],
            recv_sem=recv_sem.at[kind, me],
            device_id={"sta": peer(d)},
            device_id_type=pl.DeviceIdType.MESH,
        )
        copy.start()
        return copy

    def wait_from(kind, dst, j):
        pltpu.make_async_remote_copy(
            src_ref=dst.at[j],
            dst_ref=dst.at[j],
            send_sem=send_sem.at[kind, 0],
            recv_sem=recv_sem.at[kind, j],
            device_id={"sta": j},
            device_id_type=pl.DeviceIdType.MESH,
        ).wait_recv()

    rows = lax.broadcasted_iota(jnp.int32, (all_comb.shape[1], nt), 0)
    comb = jnp.zeros((all_comb.shape[1], nt), F32)
    for p in range(slots):
        event = jnp.where(p < counts_ref[0], events_ref[0, p], -1)
        comb = comb + jnp.where(rows == event, resid_ref[p : p + 1, :], 0.0)
    all_comb[me] = comb

    lane = lax.broadcasted_iota(jnp.int32, (LANES, LANES), 0)
    column = lax.broadcasted_iota(jnp.int32, (LANES, LANES), 1)

    def pick(j, slot):
        inside = (column >= slot * width) & (column < (slot + 1) * width)
        return inside & (lane == column + (j - slot) * width)

    def as_matrix(masks):
        return jnp.concatenate([jnp.where(m, 1.0, 0.0).astype(BF16) for m in masks], axis=0)

    def gathered(tiles, matrix):
        wide = jnp.concatenate(tiles, axis=1)
        return jnp.dot(wide, matrix[: len(tiles) * LANES], preferred_element_type=F32).astype(BF16)

    def pack_green(j, masks, matrix, dst, index):
        for a in range(full):
            dst[index, a] = gathered([green[a * per_tile + k] for k in range(per_tile)], matrix)
        if rest:
            repeated = []
            for k in range(rest):
                hit = masks[k]
                for i in range(1, fit):
                    hit = hit | masks[i * rest + k]
                repeated.append(hit)
            dst[index, full] = gathered(
                [green[full * per_tile + k] for k in range(rest)], as_matrix(repeated)
            )

    def pack_strain(matrix, dst, index):
        tile = 0
        for e in range(local_events):
            for a in range(full):
                dst[index, tile] = gathered(
                    [strain[e, a * per_tile + k] for k in range(per_tile)], matrix
                )
                tile += 1
        if rest:
            for e in range(0, local_events, fit):
                dst[index, tile] = gathered(
                    [strain[e + i, full * per_tile + k] for i in range(fit) for k in range(rest)],
                    matrix,
                )
                tile += 1

    matrices = {}
    for d in order + [0]:
        j = peer(d)
        masks = [pick(j, slot) for slot in range(per_tile)]
        matrices[d] = (j, masks, as_matrix(masks))

    load_green.wait()
    copies = []
    pl.semaphore_wait(barrier, n - 1)
    for d in order:
        copies.append(send(0, all_comb.at[me], all_comb, d))
    waiting = None
    for d in order:
        pack_green(*matrices[d], packed_green, d)
        if waiting is not None:
            copies.append(send(1, packed_green.at[waiting], all_green, waiting))
        waiting = d
    pack_green(*matrices[0], all_green, me)
    copies.append(send(1, packed_green.at[waiting], all_green, waiting))
    load_strain.wait()
    waiting = None
    for d in order:
        pack_strain(matrices[d][2], packed_strain, d)
        if waiting is not None:
            copies.append(send(2, packed_strain.at[waiting], all_strain, waiting))
        waiting = d
    pack_strain(matrices[0][2], all_strain, me)
    copies.append(send(2, packed_strain.at[waiting], all_strain, waiting))

    for d in order:
        wait_from(0, all_comb, peer(d))
    for d in order:
        wait_from(1, all_green, peer(d))

    later = column >= lane
    nothing = jnp.zeros((LANES, LANES), BF16)
    tiles = all_green.shape[1]

    @pl.loop(0, all_comb.shape[1])
    def _(e):
        total = jnp.zeros((nt, tiles * LANES), F32)
        for s in range(n):
            wave = all_comb[s, pl.ds(e, 1), :]
            turned = []
            for k in range(blocks):
                piece = jnp.broadcast_to(wave[:, k * LANES : (k + 1) * LANES], (LANES, LANES))
                turned.append(pltpu.roll(piece, 0, 1, stride=1, stride_axis=0))
            diag = [
                jnp.where(later, turned[k], turned[k - 1] if k else 0.0).astype(BF16)
                for k in range(blocks)
            ]
            matrix = jnp.concatenate(
                [
                    jnp.concatenate([nothing] * i + diag[: blocks - i], axis=1)
                    for i in range(blocks)
                ],
                axis=0,
            )
            field = jnp.concatenate([all_green[s, t] for t in range(tiles)], axis=1)
            total = total + jnp.dot(matrix, field, preferred_element_type=F32)
        adjoint[e] = total

    spot = lax.broadcasted_iota(jnp.int32, (nt, LANES), 1)

    def meet(j):
        part = jnp.zeros((1, LANES), F32)
        tile = 0
        for e in range(local_events):
            for a in range(full):
                field = all_strain[j, tile].astype(F32)
                one = adjoint[j * local_events + e, :, a * LANES : (a + 1) * LANES]
                part = part + jnp.sum(field * one, axis=0, keepdims=True)
                tile += 1
        if rest:
            for e in range(0, local_events, fit):
                field = all_strain[j, tile].astype(F32)
                one = adjoint[j * local_events + e, :, full * LANES :]
                for i in range(1, fit):
                    other = adjoint[j * local_events + e + i, :, full * LANES :]
                    one = jnp.where(spot < i * rest * width, one, other)
                part = part + jnp.sum(
                    jnp.where(spot < fit * rest * width, field * one, 0.0), axis=0, keepdims=True
                )
                tile += 1
        return part

    answer = meet(me)
    for d in order:
        j = peer(d)
        wait_from(2, all_strain, j)
        answer = answer + meet(j)
    total = answer[:, :width]
    for k in range(1, per_tile):
        total = total + answer[:, k * width : (k + 1) * width]
    out_ref[...] = total[0]
    for copy in copies:
        copy.wait_send()


def square_kernel(
    events_ref, counts_ref, resid_ref, green_hbm, strain_hbm, out_ref,
    green, strain, send_green, send_strain, own_green, far_green, own_strain, far_strain,
    own_tail, far_tail, waves, table, own_adjoint, far_adjoint, part_out, part_in,
    load_sem, send_sem, recv_sem,
):
    me = lax.axis_index("sta")
    x, y = lax.rem(me, 2), me // 2
    odd = lax.rem(x + y, 2)
    beside = me + 1 - 2 * x
    above = lax.rem(me + 2, 4)
    first = beside + odd * (above - beside)
    second = above + odd * (beside - above)
    across = 3 - me
    comps, nt, vox = green.shape
    local_events = strain.shape[0]
    width = vox // 4
    per_tile = LANES // width
    full = comps // per_tile
    rest = comps % per_tile
    blocks = nt // LANES
    head = full * nt

    load_green = pltpu.make_async_copy(green_hbm.at[0], green, load_sem.at[0])
    load_strain = pltpu.make_async_copy(strain_hbm, strain, load_sem.at[1])
    load_green.start()
    load_strain.start()

    barrier = pltpu.get_barrier_semaphore()
    for target in (first, second, across):
        pl.semaphore_signal(
            barrier, inc=1, device_id={"sta": target}, device_id_type=pl.DeviceIdType.MESH
        )

    def copy_of(kind, src, dst, target):
        return pltpu.make_async_remote_copy(
            src_ref=src,
            dst_ref=dst,
            send_sem=send_sem.at[kind],
            recv_sem=recv_sem.at[kind],
            device_id={"sta": target},
            device_id_type=pl.DeviceIdType.MESH,
        )

    plan = {
        "wave1": copy_of(0, waves.at[0], waves.at[2], first),
        "wave2": copy_of(1, waves.at[0], waves.at[1], second),
        "wave3": copy_of(2, waves.at[0], waves.at[3], across),
        "u0": copy_of(3, send_green.at[0], far_green.at[2], first),
        "u1": copy_of(4, send_strain.at[0], far_strain.at[1], first),
        "u2": copy_of(5, far_green.at[0], own_green.at[2], first),
        "u3": copy_of(6, far_green.at[2], own_green.at[3], first),
        "w0": copy_of(7, own_green.at[0], far_green.at[1], second),
        "w1": copy_of(8, send_green.at[1], own_green.at[1], second),
        "w2": copy_of(9, send_strain.at[1, 0], own_strain.at[1, 0], second),
        "w3": copy_of(12, send_strain.at[1, 1:], own_strain.at[1, 1:], second),
        "w4": copy_of(10, own_green.at[1], far_green.at[3], second),
        "sum": copy_of(11, part_out, part_in, first),
    }

    events = waves.shape[1]
    rows = lax.broadcasted_iota(jnp.int32, (events, nt), 0)
    comb = jnp.zeros((events, nt), F32)
    for p in range(resid_ref.shape[0]):
        event = jnp.where(p < counts_ref[0], events_ref[0, p], -1)
        comb = comb + jnp.where(rows == event, resid_ref[p : p + 1, :], 0.0)
    waves[0] = comb.astype(BF16)

    lane = lax.broadcasted_iota(jnp.int32, (LANES, LANES), 0)
    column = lax.broadcasted_iota(jnp.int32, (LANES, LANES), 1)

    def picker(j):
        parts = []
        for slot in range(per_tile):
            inside = (column >= slot * width) & (column < (slot + 1) * width)
            hit = inside & (lane == column + (j - slot) * width)
            parts.append(jnp.where(hit, 1.0, 0.0).astype(BF16))
        return jnp.concatenate(parts, axis=0)

    def gathered(pieces, matrix):
        wide = jnp.concatenate(pieces, axis=1)
        return jnp.dot(wide, matrix, preferred_element_type=F32).astype(BF16)

    def pack_green(matrix, dst, index):
        for a in range(full):
            dst[index, a * nt : (a + 1) * nt] = gathered(
                [green[a * per_tile + k] for k in range(per_tile)], matrix
            )
        half = nt // 2
        dst[index, head : head + half] = gathered(
            [green[full * per_tile + k, h * half : (h + 1) * half] for h in range(2) for k in range(rest)],
            matrix,
        )

    def pack_strain(matrix, dst, index):
        tile = 0
        for e in range(local_events):
            for a in range(full):
                dst[index, tile] = gathered(
                    [strain[e, a * per_tile + k] for k in range(per_tile)], matrix
                )
                tile += 1
        dst[index, tile] = gathered(
            [strain[i, full * per_tile + k] for i in range(local_events) for k in range(rest)],
            matrix,
        )

    to_across, to_second = picker(across), picker(second)
    load_green.wait()
    pack_green(to_across, send_green, 0)
    pack_green(to_second, send_green, 1)
    to_me, to_first = picker(me), picker(first)
    pl.semaphore_wait(barrier, 3)
    plan["u0"].start()
    plan["w1"].start()
    for name in ("wave3", "wave1", "wave2"):
        plan[name].start()
    load_strain.wait()
    pack_strain(to_across, send_strain, 0)
    pack_green(to_me, own_green, 0)
    plan["u1"].start()
    pack_green(to_first, far_green, 0)
    plan["w0"].start()
    pack_strain(to_second, send_strain, 1)
    plan["u2"].start()

    later = column >= lane
    low = column < rest * width
    nothing = jnp.zeros((LANES, LANES), BF16)

    def unfold(source, s, dst):
        half = nt // 2
        for b in range(half // LANES):
            piece = source[s, head + b * LANES : head + (b + 1) * LANES].astype(F32)
            turned = pltpu.roll(piece, LANES // 2, 1)
            dst[s, b * LANES : (b + 1) * LANES] = jnp.where(low, piece, turned).astype(BF16)
            dst[s, half + b * LANES : half + (b + 1) * LANES] = jnp.where(
                low, turned, piece
            ).astype(BF16)

    def toeplitz(s, row):
        wave = table[s, pl.ds(row, 1), :]
        turned = []
        for k in range(blocks):
            piece = jnp.broadcast_to(wave[:, k * LANES : (k + 1) * LANES], (LANES, LANES))
            turned.append(pltpu.roll(piece, 0, 1, stride=1, stride_axis=0))
        diag = [
            jnp.where(later, turned[k], turned[k - 1] if k else 0.0).astype(BF16)
            for k in range(blocks)
        ]
        return jnp.concatenate(
            [jnp.concatenate([nothing] * i + diag[: blocks - i], axis=1) for i in range(blocks)],
            axis=0,
        )

    def advance(source, tail, adjoint, partner, stations, fresh):
        for s in stations:
            unfold(source, s, tail)

        @pl.loop(0, 2 * local_events)
        def _(k):
            row = me * local_events + k + (k // local_events) * (partner - me - 1) * local_events
            total = jnp.zeros(adjoint.shape[1:], F32) if fresh else adjoint[k]
            for s in stations:
                field = jnp.concatenate(
                    [source[s, a * nt : (a + 1) * nt] for a in range(full)] + [tail[s]], axis=1
                )
                total = total + jnp.dot(toeplitz(s, row), field, preferred_element_type=F32)
            adjoint[k] = total

    spot = lax.broadcasted_iota(jnp.int32, (nt, LANES), 1)

    def meet(field, adjoint, side):
        part = jnp.zeros((1, LANES), F32)
        tile = 0
        base = side * local_events
        for e in range(local_events):
            for a in range(full):
                one = adjoint[base + e, :, a * LANES : (a + 1) * LANES]
                part = part + jnp.sum(field[side, tile].astype(F32) * one, axis=0, keepdims=True)
                tile += 1
        one = adjoint[base, :, full * LANES :]
        for i in range(1, local_events):
            one = jnp.where(spot < i * rest * width, one, adjoint[base + i, :, full * LANES :])
        return part + jnp.sum(field[side, tile].astype(F32) * one, axis=0, keepdims=True)

    pack_strain(to_first, far_strain, 0)
    plan["w2"].start()
    plan["u0"].wait_recv()
    plan["u3"].start()
    plan["w1"].wait_recv()
    plan["w4"].start()
    plan["w3"].start()
    pack_strain(to_me, own_strain, 0)
    for name in ("wave1", "wave2", "wave3"):
        plan[name].wait_recv()
    table[...] = waves[...].astype(F32)
    advance(own_green, own_tail, own_adjoint, first, (0, 1), True)
    plan["w0"].wait_recv()
    advance(far_green, far_tail, far_adjoint, second, (0, 1, 2), True)
    plan["w4"].wait_recv()
    advance(far_green, far_tail, far_adjoint, second, (3,), False)
    part = meet(far_strain, far_adjoint, 0)
    plan["u1"].wait_recv()
    part_out[...] = part + meet(far_strain, far_adjoint, 1)
    plan["u2"].wait_recv()
    advance(own_green, own_tail, own_adjoint, first, (2,), False)
    plan["sum"].start()
    plan["u3"].wait_recv()
    advance(own_green, own_tail, own_adjoint, first, (3,), False)
    answer = meet(own_strain, own_adjoint, 0)
    plan["w2"].wait_recv()
    plan["w3"].wait_recv()
    answer = answer + meet(own_strain, own_adjoint, 1)
    plan["sum"].wait_recv()
    answer = answer + part_in[...]
    total = answer[:, :width]
    for k in range(1, per_tile):
        total = total + answer[:, k * width : (k + 1) * width]
    out_ref[...] = total[0]
    for copy in plan.values():
        copy.wait_send()


def solution(mesh):
    n = mesh.shape["sta"]

    def body(green_tensor, strain, pair_events, pair_counts, residuals):
        _, comps, nt, vox = green_tensor.shape
        local_events = strain.shape[0]
        width = vox // n
        per_tile = LANES // width
        full = comps // per_tile
        rest = comps % per_tile
        fit = min(per_tile // rest, local_events) if rest else 1
        green_tiles = full + (1 if rest else 0)
        strain_tiles = full * local_events + (local_events // fit if rest else 0)
        events = n * local_events
        packed = full * nt + nt // 2
        if n == 4 and 2 * rest == per_tile and local_events * rest == per_tile:
            steps = square_kernel
            scratch = [
                pltpu.VMEM((comps, nt, vox), BF16),
                pltpu.VMEM((local_events, comps, nt, vox), BF16),
                pltpu.VMEM((2, packed, LANES), BF16),
                pltpu.VMEM((2, strain_tiles, nt, LANES), BF16),
                pltpu.VMEM((4, packed, LANES), BF16),
                pltpu.VMEM((4, packed, LANES), BF16),
                pltpu.VMEM((2, strain_tiles, nt, LANES), BF16),
                pltpu.VMEM((2, strain_tiles, nt, LANES), BF16),
                pltpu.VMEM((4, nt, LANES), BF16),
                pltpu.VMEM((4, nt, LANES), BF16),
                pltpu.VMEM((4, events, nt), BF16),
                pltpu.VMEM((4, events, nt), F32),
                pltpu.VMEM((2 * local_events, nt, green_tiles * LANES), F32),
                pltpu.VMEM((2 * local_events, nt, green_tiles * LANES), F32),
                pltpu.VMEM((1, LANES), F32),
                pltpu.VMEM((1, LANES), F32),
                pltpu.SemaphoreType.DMA((2,)),
                pltpu.SemaphoreType.DMA((13,)),
                pltpu.SemaphoreType.DMA((13,)),
            ]
        else:
            steps = functools.partial(kernel, n)
            scratch = [
                pltpu.VMEM((comps, nt, vox), BF16),
                pltpu.VMEM((local_events, comps, nt, vox), BF16),
                pltpu.VMEM((n, green_tiles, nt, LANES), BF16),
                pltpu.VMEM((n, strain_tiles, nt, LANES), BF16),
                pltpu.VMEM((n, events, nt), F32),
                pltpu.VMEM((n, green_tiles, nt, LANES), BF16),
                pltpu.VMEM((n, strain_tiles, nt, LANES), BF16),
                pltpu.VMEM((events, nt, green_tiles * LANES), F32),
                pltpu.SemaphoreType.DMA((2,)),
                pltpu.SemaphoreType.DMA((3, n)),
                pltpu.SemaphoreType.DMA((3, n)),
            ]
        return pl.pallas_call(
            steps,
            out_shape=jax.ShapeDtypeStruct((width,), F32),
            in_specs=[
                pl.BlockSpec(memory_space=pltpu.SMEM),
                pl.BlockSpec(memory_space=pltpu.SMEM),
                pl.BlockSpec(memory_space=pltpu.VMEM),
                pl.BlockSpec(memory_space=pl.ANY),
                pl.BlockSpec(memory_space=pl.ANY),
            ],
            out_specs=pl.BlockSpec(memory_space=pltpu.VMEM),
            scratch_shapes=scratch,
            compiler_params=pltpu.CompilerParams(collective_id=0, has_side_effects=True),
        )(pair_events, pair_counts, residuals[0], green_tensor, strain)

    in_specs = (
        P("sta", None, None, "vox"),
        P("sta", None, None, "vox"),
        P("sta", None),
        P("sta"),
        P("sta", None, None),
    )
    out_specs = P(("vox", "sta"))
    return jax.shard_map(body, mesh=mesh, in_specs=in_specs, out_specs=out_specs, check_vma=False)
```
